64 devices in a mesh: dp: 8 (over x, y, core), sp: 8 (over z).
Axes of the slice: x: 2, y: 2, z: 8, core: 2. Of those that a mesh axis runs over, the one named last changes fastest.
The devices are a block of a 4x4x8 slice.
Arguments:
- x: bfloat16 [65536, 2048], P(('dp', 'sp')), parts along dimension 0
- gain: bfloat16 [2048], replicated
- wq: bfloat16 [2048, 2048], P('sp')
- wk: bfloat16 [2048, 256], P('sp')
- wv: bfloat16 [2048, 256], P('sp')
- wo: bfloat16 [2048, 2048], P('sp')
Outputs:
- output: bfloat16 [65536, 2048], P(('dp', 'sp')), parts along dimension 0
There are 8 independent parts. The reference program is written for one: setup_inputs(seed, part) draws one part's arguments, and reference() takes and returns one part's arrays. A program takes and returns all parts, laid end to end along the dimension named above; an argument that names none is the same for every part.
All inputs are finite; a program needn't handle non-finite values.
Results may differ from the reference program's by a relative error of at most 0.012.
Values are sent between devices in bfloat16 or wider.
A program may use at most 768 MiB of HBM per device.

```python
import jax
import jax.numpy as jnp
from jax import lax

ROWS = 8192
D = 2048
HEADS = 8
KV_HEADS = 1
HEAD = 256
THETA = 10000


def setup_inputs(seed: int = 0, part: int = 0) -> dict:
    kx, kn, kq, kk, kv, ko = jax.random.split(jax.random.key(seed), 6)

    def weights(key, rows, columns):
        return jax.random.normal(key, (rows, columns), jnp.float32) * rows**-0.5

    drawn = {
        "x": jax.random.normal(jax.random.fold_in(kx, part), (ROWS, D), jnp.float32),
        "gain": 1 + 0.1 * jax.random.normal(kn, (D,), jnp.float32),
        "wq": 2 * weights(kq, D, HEADS * HEAD),
        "wk": 2 * weights(kk, D, KV_HEADS * HEAD),
        "wv": 4 * weights(kv, D, KV_HEADS * HEAD),
        "wo": weights(ko, HEADS * HEAD, D),
    }
    return {k: v.astype(jnp.bfloat16) for k, v in drawn.items()}


def normed(x, gain):
    wide = x.astype(jnp.float32)
    scale = lax.rsqrt(jnp.mean(wide * wide, -1, keepdims=True) + 1e-6)
    return (wide * scale * gain.astype(jnp.float32)).astype(jnp.bfloat16)


def turned(t, place, theta):
    half = t.shape[-1] // 2
    angle = place.astype(jnp.float32)[:, None] * theta ** (-jnp.arange(half, dtype=jnp.float32) / half)
    cos, sin = jnp.cos(angle)[:, None], jnp.sin(angle)[:, None]
    a, b = t[..., :half].astype(jnp.float32), t[..., half:].astype(jnp.float32)
    return jnp.concatenate([a * cos - b * sin, b * cos + a * sin], -1).astype(jnp.bfloat16)


def matmul(a, w):
    return jnp.dot(a, w, preferred_element_type=jnp.float32).astype(jnp.bfloat16)


def einsum(form, a, b):
    return jnp.einsum(form, a.astype(jnp.float32), b.astype(jnp.float32))


def attention(q, k, v):
    scores = einsum("tgsd,ugd->gstu", q, k) * q.shape[-1] ** -0.5
    token = jnp.arange(q.shape[0])
    scores = jnp.where(token[:, None] >= token, scores, -jnp.inf)
    weights = jax.nn.softmax(scores, -1).astype(jnp.bfloat16)
    return einsum("gstu,ugd->tgsd", weights, v).astype(jnp.bfloat16)


def reference(x, gain, wq, wk, wv, wo):
    a, place = normed(x, gain), jnp.arange(ROWS)
    q = turned(matmul(a, wq).reshape(ROWS, HEADS, HEAD), place, THETA).reshape(ROWS, KV_HEADS, -1, HEAD)
    k = turned(matmul(a, wk).reshape(ROWS, KV_HEADS, HEAD), place, THETA)
    v = matmul(a, wv).reshape(ROWS, KV_HEADS, HEAD)
    seen = attention(q, k, v).reshape(ROWS, HEADS * HEAD)
    return (x.astype(jnp.float32) + jnp.dot(seen, wo, preferred_element_type=jnp.float32)).astype(jnp.bfloat16)
```

```python
import functools

import jax
import jax.numpy as jnp
from jax import lax
from jax.experimental import pallas as pl
from jax.experimental.pallas import tpu as pltpu
from jax.sharding import PartitionSpec as P

HEAD = 256
THETA = 10000
NEG = -1e30
HIDDEN = 2 * NEG
LOG2E = 1.4426950408889634
MESH = pl.DeviceIdType.MESH
f32, bf16 = jnp.float32, jnp.bfloat16

UNIT = 512
BLOCK = 128
PART = 512
START = {0: 0, 1: 1, 2: 2, 3: 3, 4: 4}


def _dot(a, b, ca=1, cb=0):
    return lax.dot_general(a, b, (((ca,), (cb,)), ((), ())), preferred_element_type=f32)


def _fused(ns, nq, x_hbm, gain_ref, cos_ref, sin_ref, wq_hbm, wk_hbm, wv_hbm, wo_hbm, out_hbm,
           a_s, q_s, k_s, v_s, w_s, mix_s, top_s, x_sem, load_sem, out_sem, z_send, z_recv, y_send, y_recv, c_send, c_recv,
           kv_send, kv_recv):
    own, width = a_s.shape
    rows = wq_hbm.shape[0]
    parts = own // PART
    nh = q_s.shape[2] // PART
    nu = nq // UNIT
    far, near = ns // 2, ns - 1 - ns // 2
    z, g = lax.axis_index("sp"), lax.axis_index("dp")
    core, yp = lax.rem(g, 2), lax.rem(lax.div(g, 2), 2)
    right, left = {"sp": lax.rem(z + 1, ns)}, {"sp": lax.rem(z + ns - 1, ns)}
    twin = {"dp": g + 1 - 2 * core}
    pair = {"dp": g + 2 - 4 * yp}

    def at(d):
        return lax.rem(z + d + ns, ns)

    def piece(u, k, s):
        return w_s.at[u, pl.ds(pl.multiple_of(s * rows, rows), rows), pl.ds(pl.multiple_of(k * BLOCK, BLOCK), BLOCK)]

    def send(src, dst, s_sem, r_sem, to):
        return pltpu.make_async_remote_copy(src_ref=src, dst_ref=dst, send_sem=s_sem, recv_sem=r_sem, device_id=to, device_id_type=MESH)

    def slots(u):
        if u == 0:
            return [(0, 0, core, far, near, False), (2 * nu + 1, 0, core + 2, near, far, False)]
        r, l = (far, near) if u % 2 else (near, far)
        return [(u, u, 2 * yp + core, r, l, True)]

    def hop(slot, u, k, h, way):
        s = at(1 - h) if way == 0 else at(h - 1)
        return send(piece(u, k, s), piece(u, k, s), z_send.at[slot], z_recv.at[slot, way, h - 1], right if way == 0 else left)

    def came(slot, u, k, h, way):
        s = at(-h) if way == 0 else at(h)
        p = piece(u, k, s)
        return send(p, p, z_send.at[slot], z_recv.at[slot, way, h - 1], right), p

    def ring_send(u, h):
        for slot, u, k, r, l, _ in slots(u):
            if h <= r:
                hop(slot, u, k, h, 0).start()
            if h <= l:
                hop(slot, u, k, h, 1).start()

    def hand_on(u, p, shared):
        if shared:
            send(p, p, y_send.at[u], y_recv.at[u], pair).start()
        send(p, p, c_send.at[u], c_recv.at[u], twin).start()

    def ring_step(u, h):
        for slot, u, k, r, l, shared in slots(u):
            for way, n in ((0, r), (1, l)):
                if h <= n:
                    c, p = came(slot, u, k, h, way)
                    c.wait_recv()
                    if h < n:
                        hop(slot, u, k, h + 1, way).start()
                    hand_on(u, p, shared)

    def bulk(u, pieces):
        return w_s.at[u, pl.ds(0, pieces * rows // 2), pl.ds(0, 2 * BLOCK)]

    def from_pair(u):
        send(bulk(u, ns - 1), bulk(u, ns - 1), y_send.at[u], y_recv.at[u], pair).wait_recv()
        k = 2 * (1 - yp) + core
        for d in range(1, ns):
            p = piece(u, k, at(d))
            send(p, p, c_send.at[u], c_recv.at[u], twin).start()

    def whole(u):
        send(bulk(u, 2 * (ns - 1)), bulk(u, 2 * (ns - 1)), c_send.at[u], c_recv.at[u], twin).wait_recv()

    def sent(u):
        for slot, *_ in slots(u):
            send(bulk(u, ns - 1), bulk(u, ns - 1), z_send.at[slot], z_recv.at[slot, 0, 0], right).wait_send()
        if u:
            send(bulk(u, ns - 1), bulk(u, ns - 1), y_send.at[u], y_recv.at[u], pair).wait_send()
        send(bulk(u, 2 * (ns - 1)), bulk(u, 2 * (ns - 1)), c_send.at[u], c_recv.at[u], twin).wait_send()

    def kv_copies(a, way, s):
        p = lax.rem(a + way, 2)
        to = right if way == 0 else left
        return [send(ref.at[s, p], ref.at[s, p], kv_send.at[i], kv_recv.at[i, way, a], to) for i, ref in enumerate((k_s, v_s))]

    def kv_start(a):
        h = lax.div(a, 2) + 1
        for way, s in ((0, at(1 - h)), (1, at(h - 1))):
            for c in kv_copies(a, way, s):
                c.start()

    def kv_wait(a):
        h = lax.div(a, 2) + 1
        for way, s in ((0, at(-h)), (1, at(h))):
            for c in kv_copies(a, way, s):
                c.wait_recv()

    kv_rounds = parts * (ns - 1) // 2

    def load(u, k):
        if u == 0:
            src, c = (wk_hbm, k) if k < 2 else (wv_hbm, k - 2)
        elif u <= nu:
            src, c = wq_hbm, 4 * (u - 1) + k
        else:
            src, c = wo_hbm, 4 * (u - 1 - nu) + k
        return pltpu.make_async_copy(src.at[:, pl.ds(c * BLOCK, BLOCK)], piece(u, k, z), load_sem.at[u, k])

    units = range(1 + 2 * nu)
    blocks = UNIT // BLOCK
    xt = own // x_sem.shape[0]
    xs = [pltpu.make_async_copy(x_hbm.at[pl.ds(t * xt, xt)], a_s.at[pl.ds(t * xt, xt)], x_sem.at[t]) for t in range(x_sem.shape[0])]
    for k in range(blocks):
        load(0, k).start()
    for c in xs:
        c.start()
    for u in units[1:]:
        for k in range(blocks):
            load(u, k).start()

    barrier = pltpu.get_barrier_semaphore()
    for to in (left, right, twin, pair):
        pl.semaphore_signal(barrier, inc=1, device_id=to, device_id_type=MESH)
    pl.semaphore_wait(barrier, 4)

    def loaded(u):
        for k in range(blocks):
            load(u, k).wait()

    loaded(0)
    ring_send(0, 1)

    for c in xs:
        c.wait()

    def norm(t, _):
        r = pl.ds(pl.multiple_of(t * 128, 128), 128)
        wide = a_s[r, :].astype(f32)
        scale = lax.rsqrt(jnp.mean(wide * wide, -1, keepdims=True) + 1e-6)
        a_s[r, :] = (wide * scale * gain_ref[...].astype(f32)).astype(bf16)

    lax.fori_loop(0, own // 128, norm, None)
    top_s[...] = jnp.full(top_s.shape, NEG, f32)

    def clear(i, _):
        mix_s[lax.div(i, nh), :, pl.ds(pl.multiple_of(lax.rem(i, nh) * PART, PART), PART)] = jnp.zeros((mix_s.shape[1], PART), f32)

    lax.fori_loop(0, parts * nh, clear, None)

    def turned(t, r):
        half = HEAD // 2
        c, s = cos_ref[r, :], sin_ref[r, :]
        t = t.astype(bf16).astype(f32)
        a, b = t[:, :half], t[:, half:]
        return jnp.concatenate([a * c - b * s, b * c + a * s], axis=1).astype(bf16)

    def keys_values():
        def one(p, _):
            r = pl.ds(pl.multiple_of(p * PART, PART), PART)
            t = _dot(a_s[r, :], w_s[0])
            k_s[z, p] = turned(t[:, :HEAD], r)
            v_s[z, p] = t[:, HEAD:].T.astype(bf16)

        lax.fori_loop(0, parts, one, None)

    def queries(u):
        def one(p, _):
            r = pl.ds(pl.multiple_of(p * PART, PART), PART)
            t = _dot(a_s[r, :], w_s[u])
            for i in range(UNIT // HEAD):
                head = (u - 1) * (UNIT // HEAD) + i
                q_s[p, :, head * PART : (head + 1) * PART] = turned(t[:, i * HEAD : (i + 1) * HEAD], r).astype(f32).T.astype(bf16)

        lax.fori_loop(0, parts, one, None)

    e = HEAD**-0.5 * LOG2E

    def tile(s, p, iq, masked):
        key = k_s[s, p]
        value = jnp.concatenate([v_s[s, p], jnp.ones((8, PART), bf16)], axis=0)
        cut = [pl.ds(h * PART, PART) for h in range(nh)]
        scores = [_dot(key, q_s[iq, :, c]) for c in cut]
        if masked:
            seen = lax.broadcasted_iota(jnp.int32, (PART, PART), 1) >= lax.broadcasted_iota(jnp.int32, (PART, PART), 0)
        weights, keeps = [], []
        for c, sc in zip(cut, scores):
            if masked:
                sc = jnp.where(seen, sc, HIDDEN)
            old = top_s[iq, :, c]
            top = jnp.maximum(old, sc.max(axis=0, keepdims=True))
            top_s[iq, :, c] = top
            weights.append(jnp.exp2((sc - top) * e).astype(bf16))
            keeps.append(jnp.exp2((old - top) * e))
        for c, w, keep in zip(cut, weights, keeps):
            mix_s[iq, :, c] = mix_s[iq, :, c] * keep + _dot(value, w)

    last = max(START.values()) + 7
    for r in range(1, last):
        for u, start in START.items():
            if start == r:
                loaded(u)
                ring_send(u, 1)
            elif 1 <= r - start <= far:
                ring_step(u, r - start)
            elif r - start == far + 1 and u:
                from_pair(u)
        for u, start in START.items():
            if u == 0 and r == far:
                whole(0)
                keys_values()
                kv_start(0)
                kv_start(1)
            elif u and r - start == far + 2:
                whole(u)
                queries(u)

    lax.fori_loop(0, parts, lambda p, _: tile(z, p, p, True), None)
    for p in range(parts):
        for iq in range(p + 1, parts):
            tile(z, p, iq, False)

    half = own
    per = w_s.shape[1] // half

    def x_place(c):
        return w_s.at[1 + c // per, pl.ds((c % per) * half, half)]

    again = [pltpu.make_async_copy(x_hbm.at[:, pl.ds(c * UNIT, UNIT)], x_place(c), load_sem.at[1 + c // blocks, c % blocks]) for c in range(width // UNIT)]
    for u in range(1, 1 + len(again) // per):
        sent(u)
    for u in range(1 + nu, 1 + 2 * nu):
        loaded(u)
    for c in again:
        c.start()

    outs = [(1 + nu + i, i // 2) for i in range(nu)]

    def round_(a, _):
        kv_wait(a)

        @pl.when(a + 2 < kv_rounds)
        def _():
            kv_start(a + 2)

        for u, first in outs:
            for h in range(far + 2):
                @pl.when(a - first == h)
                def _():
                    if h == 0:
                        ring_send(u, 1)
                    elif h <= far:
                        ring_step(u, h)
                    else:
                        from_pair(u)

        h = lax.div(a, 2) + 1

        def some(i, _):
            way, iq = lax.div(i, parts), lax.rem(i, parts)
            s = jnp.where(way == 0, at(-h), at(h))

            @pl.when(s < z)
            def _():
                tile(s, lax.rem(a + way, 2), iq, False)

        lax.fori_loop(0, 2 * parts, some, None)

    lax.fori_loop(0, kv_rounds, round_, None)

    def finish(p, _):
        r = pl.ds(pl.multiple_of(p * PART, PART), PART)
        for h in range(nh):
            c = pl.ds(h * PART, PART)
            a_s[r, h * HEAD : (h + 1) * HEAD] = (mix_s[p, :HEAD, c] * (1 / mix_s[p, HEAD : HEAD + 1, c])).T.astype(bf16)

    lax.fori_loop(0, parts, finish, None)
    for c in again:
        c.wait()
    for u, _ in outs:
        whole(u)

    def result(i, _):
        c, p = lax.div(i, parts), lax.rem(i, parts)
        r = pl.ds(pl.multiple_of(p * PART, PART), PART)
        place = w_s.at[1 + lax.div(c, per), pl.ds(pl.multiple_of(lax.rem(c, per) * half + p * PART, PART), PART)]
        place[...] = (place[...].astype(f32) + _dot(a_s[r, :], w_s[1 + nu + c])).astype(bf16)
        pltpu.make_async_copy(place, out_hbm.at[r, pl.ds(pl.multiple_of(c * UNIT, UNIT), UNIT)], out_sem).start()

    lax.fori_loop(0, parts * (width // UNIT), result, None)

    for u in units:
        if u == 0 or u > len(again) // per:
            sent(u)
    for i, ref in enumerate((k_s, v_s)):
        send(ref.at[pl.ds(0, ns - 1)], ref.at[pl.ds(0, ns - 1)], kv_send.at[i], kv_recv.at[i, 0, 0], right).wait_send()
    pltpu.make_async_copy(a_s, out_hbm, out_sem).wait()


def solution(mesh):
    ns = mesh.shape["sp"]

    def step(x, gain, wq, wk, wv, wo):
        own, width = x.shape
        nq = wq.shape[1]
        nh = nq // HEAD
        nu = nq // UNIT
        parts = own // PART
        place = lax.axis_index("sp") * own + jnp.arange(own)
        half = HEAD // 2
        angle = place.astype(f32)[:, None] * THETA ** (-jnp.arange(half, dtype=f32) / half)
        cos, sin = jnp.cos(angle), jnp.sin(angle)
        anywhere = pl.BlockSpec(memory_space=pl.ANY)
        vmem = pl.BlockSpec(memory_space=pltpu.VMEM)
        dma = pltpu.SemaphoreType.DMA
        slots = 2 * nu + 2
        return pl.pallas_call(
            functools.partial(_fused, ns, nq),
            out_shape=jax.ShapeDtypeStruct(x.shape, x.dtype),
            in_specs=[anywhere, vmem, vmem, vmem] + [anywhere] * 4,
            out_specs=anywhere,
            scratch_shapes=[
                pltpu.VMEM((own, width), bf16),
                pltpu.VMEM((parts, HEAD, nh * PART), bf16),
                pltpu.VMEM((ns, parts, PART, HEAD), bf16),
                pltpu.VMEM((ns, parts, HEAD, PART), bf16),
                pltpu.VMEM((1 + 2 * nu, width, UNIT), bf16),
                pltpu.VMEM((parts, HEAD + 8, nh * PART), f32),
                pltpu.VMEM((parts, 1, nh * PART), f32),
                dma((4,)),
                dma((1 + 2 * nu, UNIT // BLOCK)),
                dma,
                dma((slots,)),
                dma((slots, 2, ns // 2)),
                dma((slots,)),
                dma((slots,)),
                dma((slots,)),
                dma((slots,)),
                dma((2,)),
                dma((2, 2, parts * (ns - 1) // 2)),
            ],
            compiler_params=pltpu.CompilerParams(collective_id=0, has_side_effects=True, vmem_limit_bytes=67043328),
        )(x, gain.reshape(1, width), cos, sin, wq, wk, wv, wo)

    tokens, rows = P(("dp", "sp"), None), P("sp", None)
    return jax.shard_map(step, mesh=mesh, in_specs=(tokens, P(None), rows, rows, rows, rows), out_specs=tokens, check_vma=False)
```

```python
import functools

import jax
import jax.numpy as jnp
from jax import lax
from jax.experimental import pallas as pl
from jax.experimental.pallas import tpu as pltpu
from jax.sharding import PartitionSpec as P

HEAD = 256
THETA = 10000
NEG = -1e30
HIDDEN = 2 * NEG
LOG2E = 1.4426950408889634
MESH = pl.DeviceIdType.MESH
f32, bf16 = jnp.float32, jnp.bfloat16

UNIT = 512
BLOCK = 128
PART = 512
START = {0: 0, 2: 0, 3: 1, 4: 2, 1: 3}
OUT_HOPS = (2, 6, 10, 12, 13)
TWIN_ONLY = (0, 1)


def _dot(a, b, ca=1, cb=0):
    return lax.dot_general(a, b, (((ca,), (cb,)), ((), ())), preferred_element_type=f32)


def _fused(ns, nq, x_hbm, gain_ref, rate_ref, wq_hbm, wk_hbm, wv_hbm, wo_hbm, out_hbm,
           a_s, q_s, k_s, v_s, w_s, mix_s, top_s, cos_s, sin_s, x_sem, load_sem, out_sem, z_send, z_recv, y_send, y_recv, c_send, c_recv,
           kv_send, kv_recv):
    own, width = a_s.shape
    rows = wq_hbm.shape[0]
    parts = own // PART
    nh = q_s.shape[2] // PART
    nu = nq // UNIT
    far, near = ns // 2, ns - 1 - ns // 2
    z, g = lax.axis_index("sp"), lax.axis_index("dp")
    core, yp = lax.rem(g, 2), lax.rem(lax.div(g, 2), 2)
    right, left = {"sp": lax.rem(z + 1, ns)}, {"sp": lax.rem(z + ns - 1, ns)}
    twin = {"dp": g + 1 - 2 * core}
    pair = {"dp": g + 2 - 4 * yp}

    def at(d):
        return lax.rem(z + d + ns, ns)

    def piece(u, k, s):
        return w_s.at[u, pl.ds(pl.multiple_of(s * rows, rows), rows), pl.ds(pl.multiple_of(k * BLOCK, BLOCK), BLOCK)]

    def send(src, dst, s_sem, r_sem, to):
        return pltpu.make_async_remote_copy(src_ref=src, dst_ref=dst, send_sem=s_sem, recv_sem=r_sem, device_id=to, device_id_type=MESH)

    def slots(u):
        if u in TWIN_ONLY:
            return [(u, u, core, far, near, False), (1 + 2 * nu + u, u, core + 2, near, far, False)]
        r, l = (far, near) if u % 2 else (near, far)
        return [(u, u, 2 * yp + core, r, l, True)]

    def hop(slot, u, k, h, way):
        s = at(1 - h) if way == 0 else at(h - 1)
        return send(piece(u, k, s), piece(u, k, s), z_send.at[slot], z_recv.at[slot, way, h - 1], right if way == 0 else left)

    def came(slot, u, k, h, way):
        s = at(-h) if way == 0 else at(h)
        p = piece(u, k, s)
        return send(p, p, z_send.at[slot], z_recv.at[slot, way, h - 1], right), p

    def ring_send(u, h):
        for slot, u, k, r, l, _ in slots(u):
            if h <= r:
                hop(slot, u, k, h, 0).start()
            if h <= l:
                hop(slot, u, k, h, 1).start()

    def hand_on(u, p, shared):
        if shared:
            send(p, p, y_send.at[u], y_recv.at[u], pair).start()
        send(p, p, c_send.at[u], c_recv.at[u], twin).start()

    def ring_step(u, h):
        for slot, u, k, r, l, shared in slots(u):
            for way, n in ((0, r), (1, l)):
                if h <= n:
                    c, p = came(slot, u, k, h, way)
                    c.wait_recv()
                    if h < n:
                        hop(slot, u, k, h + 1, way).start()
                    hand_on(u, p, shared)

    def bulk(u, pieces):
        return w_s.at[u, pl.ds(0, pieces * rows // 2), pl.ds(0, 2 * BLOCK)]

    def from_pair(u):
        send(bulk(u, ns - 1), bulk(u, ns - 1), y_send.at[u], y_recv.at[u], pair).wait_recv()
        k = 2 * (1 - yp) + core
        for d in range(1, ns):
            p = piece(u, k, at(d))
            send(p, p, c_send.at[u], c_recv.at[u], twin).start()

    def whole(u):
        send(bulk(u, 2 * (ns - 1)), bulk(u, 2 * (ns - 1)), c_send.at[u], c_recv.at[u], twin).wait_recv()

    def sent(u):
        for slot, *_ in slots(u):
            send(bulk(u, ns - 1), bulk(u, ns - 1), z_send.at[slot], z_recv.at[slot, 0, 0], right).wait_send()
        if u not in TWIN_ONLY:
            send(bulk(u, ns - 1), bulk(u, ns - 1), y_send.at[u], y_recv.at[u], pair).wait_send()
        send(bulk(u, 2 * (ns - 1)), bulk(u, 2 * (ns - 1)), c_send.at[u], c_recv.at[u], twin).wait_send()

    def kv_copies(a, way, s):
        p = lax.rem(a + way, 2)
        to = right if way == 0 else left
        return [send(ref.at[s, p], ref.at[s, p], kv_send.at[i], kv_recv.at[i, way, a], to) for i, ref in enumerate((k_s, v_s))]

    def kv_start(a):
        h = lax.div(a, 2) + 1
        for way, s in ((0, at(1 - h)), (1, at(h - 1))):
            for c in kv_copies(a, way, s):
                c.start()

    def kv_wait(a):
        h = lax.div(a, 2) + 1
        for way, s in ((0, at(-h)), (1, at(h))):
            for c in kv_copies(a, way, s):
                c.wait_recv()

    kv_rounds = parts * (ns - 1) // 2

    def load(u, k):
        if u == 0:
            src, c = (wk_hbm, k) if k < 2 else (wv_hbm, k - 2)
        elif u <= nu:
            src, c = wq_hbm, 4 * (u - 1) + k
        else:
            src, c = wo_hbm, 4 * (u - 1 - nu) + k
        return pltpu.make_async_copy(src.at[:, pl.ds(c * BLOCK, BLOCK)], piece(u, k, z), load_sem.at[u, k])

    units = range(1 + 2 * nu)
    blocks = UNIT // BLOCK
    xt = own // x_sem.shape[0]
    xs = [pltpu.make_async_copy(x_hbm.at[pl.ds(t * xt, xt)], a_s.at[pl.ds(t * xt, xt)], x_sem.at[t]) for t in range(x_sem.shape[0])]
    for k in range(blocks):
        load(0, k).start()
    for c in xs:
        c.start()
    for u in units[1:]:
        for k in range(blocks):
            load(u, k).start()

    barrier = pltpu.get_barrier_semaphore()
    for to in (left, right, twin, pair):
        pl.semaphore_signal(barrier, inc=1, device_id=to, device_id_type=MESH)
    pl.semaphore_wait(barrier, 4)

    def loaded(u):
        for k in range(blocks):
            load(u, k).wait()

    for u, start in START.items():
        if start == 0:
            loaded(u)
            ring_send(u, 1)

    for c in xs:
        c.wait()

    def norm(t, _):
        r = pl.ds(pl.multiple_of(t * 128, 128), 128)
        wide = a_s[r, :].astype(f32)
        scale = lax.rsqrt(jnp.mean(wide * wide, -1, keepdims=True) + 1e-6)
        a_s[r, :] = (wide * scale * gain_ref[...].astype(f32)[None]).astype(bf16)

    lax.fori_loop(0, own // 128, norm, None)
    top_s[...] = jnp.full(top_s.shape, NEG, f32)

    def clear(i, _):
        mix_s[lax.div(i, nh), :, pl.ds(pl.multiple_of(lax.rem(i, nh) * PART, PART), PART)] = jnp.zeros((mix_s.shape[1], PART), f32)

    lax.fori_loop(0, parts * nh, clear, None)

    def angles(t, _):
        r = pl.ds(pl.multiple_of(t * 128, 128), 128)
        place = z * own + t * 128 + lax.broadcasted_iota(jnp.int32, (128, HEAD // 2), 0)
        angle = place.astype(f32) * rate_ref[...]
        cos_s[r, :] = jnp.cos(angle)
        sin_s[r, :] = jnp.sin(angle)

    lax.fori_loop(0, own // 128, angles, None)

    def turned(t, r):
        half = HEAD // 2
        c, s = cos_s[r, :], sin_s[r, :]
        t = t.astype(bf16).astype(f32)
        a, b = t[:, :half], t[:, half:]
        return jnp.concatenate([a * c - b * s, b * c + a * s], axis=1).astype(bf16)

    def keys_values():
        def one(p, _):
            r = pl.ds(pl.multiple_of(p * PART, PART), PART)
            t = _dot(a_s[r, :], w_s[0])
            k_s[z, p] = turned(t[:, :HEAD], r)
            v_s[z, p] = t[:, HEAD:].T.astype(bf16)

        lax.fori_loop(0, parts, one, None)

    def queries(u):
        def one(p, _):
            r = pl.ds(pl.multiple_of(p * PART, PART), PART)
            t = _dot(a_s[r, :], w_s[u])
            for i in range(UNIT // HEAD):
                head = (u - 1) * (UNIT // HEAD) + i
                q_s[p, :, head * PART : (head + 1) * PART] = turned(t[:, i * HEAD : (i + 1) * HEAD], r).astype(f32).T.astype(bf16)

        lax.fori_loop(0, parts, one, None)

    e = HEAD**-0.5 * LOG2E

    cuts = [pl.ds(h * PART, PART) for h in range(nh)]

    def tile(s, n, iq, masked):
        key = k_s[s, 0:n].reshape(n * PART, HEAD)
        value = jnp.concatenate([v_s[s, p] for p in range(n)], axis=1)
        value = jnp.concatenate([value, jnp.ones((8, n * PART), bf16)], axis=0)
        if masked:
            seen = iq * PART + lax.broadcasted_iota(jnp.int32, (n * PART, PART), 1) >= lax.broadcasted_iota(jnp.int32, (n * PART, PART), 0)
        scores, weights = {}, {}
        for i in range(nh + 2):
            if i < nh:
                scores[i] = _dot(key, q_s[iq, :, cuts[i]])
            j = i - 1
            if 0 <= j < nh:
                c, sc = cuts[j], scores.pop(j)
                if masked:
                    sc = jnp.where(seen, sc, HIDDEN)
                old = top_s[iq, :, c]
                top = jnp.maximum(old, sc.max(axis=0, keepdims=True))
                top_s[iq, :, c] = top
                weights[j] = jnp.exp2((sc - top) * e).astype(bf16), jnp.exp2((old - top) * e)
            j = i - 2
            if 0 <= j < nh:
                c, (w, keep) = cuts[j], weights.pop(j)
                mix_s[iq, :, c] = mix_s[iq, :, c] * keep + _dot(value, w)

    rounds = max(START.values()) + far
    for r in range(1, rounds + 1):
        for u, start in START.items():
            if start == r:
                loaded(u)
                ring_send(u, 1)
            elif 1 <= r - start <= far:
                ring_step(u, r - start)
        if r == far:
            whole(0)
            keys_values()
        if r == rounds - 2:
            from_pair(2)
        if r == rounds - 1:
            kv_start(0)
            kv_start(1)
            whole(2)
            queries(2)
    from_pair(3)
    whole(1)
    queries(1)
    from_pair(4)
    whole(3)
    queries(3)
    whole(4)
    queries(4)

    for p in range(parts):
        tile(z, p + 1, p, True)

    half = own
    per = w_s.shape[1] // half

    def x_place(c):
        return w_s.at[1 + c // per, pl.ds((c % per) * half, half)]

    again = [pltpu.make_async_copy(x_hbm.at[:, pl.ds(c * UNIT, UNIT)], x_place(c), load_sem.at[1 + c // blocks, c % blocks]) for c in range(width // UNIT)]
    for u in range(1, 1 + len(again) // per):
        sent(u)
    for u in range(1 + nu, 1 + 2 * nu):
        loaded(u)
    for c in again:
        c.start()

    outs = range(1 + nu, 1 + 2 * nu)

    def out_hop(h):
        for u in outs:
            if h:
                ring_step(u, h)
            else:
                ring_send(u, 1)

    def step(t, _):
        a, iq = lax.div(t, parts), lax.rem(t, parts)
        fresh = iq == 0

        @pl.when(fresh & (a + 1 < kv_rounds))
        def _():
            kv_wait(a + 1)

        for h, when in enumerate(OUT_HOPS):
            pl.when(t == when)(functools.partial(out_hop, h))

        @pl.when(fresh & (a + 3 < kv_rounds))
        def _():
            kv_start(a + 3)

        h = lax.div(a, 2) + 1
        s = jnp.where(lax.rem(a, 2) == 0, at(-h), at(h))

        @pl.when(s < z)
        def _():
            tile(s, parts, iq, False)

    kv_wait(0)
    kv_start(2)
    lax.fori_loop(0, parts * kv_rounds, step, None)

    def finish(p, _):
        r = pl.ds(pl.multiple_of(p * PART, PART), PART)
        for h in range(nh):
            c = pl.ds(h * PART, PART)
            a_s[r, h * HEAD : (h + 1) * HEAD] = (mix_s[p, :HEAD, c] * (1 / mix_s[p, HEAD : HEAD + 1, c])).T.astype(bf16)

    lax.fori_loop(0, parts, finish, None)
    for c in again:
        c.wait()
    for u in outs:
        from_pair(u)
    for u in outs:
        whole(u)

    def result(i, _):
        c, p = lax.div(i, parts), lax.rem(i, parts)
        r = pl.ds(pl.multiple_of(p * PART, PART), PART)
        place = w_s.at[1 + lax.div(c, per), pl.ds(pl.multiple_of(lax.rem(c, per) * half + p * PART, PART), PART)]
        place[...] = (place[...].astype(f32) + _dot(a_s[r, :], w_s[1 + nu + c])).astype(bf16)
        pltpu.make_async_copy(place, out_hbm.at[r, pl.ds(pl.multiple_of(c * UNIT, UNIT), UNIT)], out_sem).start()

    lax.fori_loop(0, parts * (width // UNIT), result, None)

    for u in units:
        if u == 0 or u > len(again) // per:
            sent(u)
    for i, ref in enumerate((k_s, v_s)):
        send(ref.at[pl.ds(0, ns - 1)], ref.at[pl.ds(0, ns - 1)], kv_send.at[i], kv_recv.at[i, 0, 0], right).wait_send()
    pltpu.make_async_copy(a_s, out_hbm, out_sem).wait()


def solution(mesh):
    ns = mesh.shape["sp"]

    def step(x, gain, wq, wk, wv, wo):
        own, width = x.shape
        nq = wq.shape[1]
        nh = nq // HEAD
        nu = nq // UNIT
        parts = own // PART
        half = HEAD // 2
        rate = THETA ** (-jnp.arange(half, dtype=f32) / half)
        anywhere = pl.BlockSpec(memory_space=pl.ANY)
        vmem = pl.BlockSpec(memory_space=pltpu.VMEM)
        dma = pltpu.SemaphoreType.DMA
        slots = 1 + 2 * nu + len(TWIN_ONLY)
        return pl.pallas_call(
            functools.partial(_fused, ns, nq),
            out_shape=jax.ShapeDtypeStruct(x.shape, x.dtype),
            in_specs=[anywhere, vmem, vmem] + [anywhere] * 4,
            out_specs=anywhere,
            scratch_shapes=[
                pltpu.VMEM((own, width), bf16),
                pltpu.VMEM((parts, HEAD, nh * PART), bf16),
                pltpu.VMEM((ns, parts, PART, HEAD), bf16),
                pltpu.VMEM((ns, parts, HEAD, PART), bf16),
                pltpu.VMEM((1 + 2 * nu, width, UNIT), bf16),
                pltpu.VMEM((parts, HEAD + 8, nh * PART), f32),
                pltpu.VMEM((parts, 1, nh * PART), f32),
                pltpu.VMEM((own, HEAD // 2), f32),
                pltpu.VMEM((own, HEAD // 2), f32),
                dma((4,)),
                dma((1 + 2 * nu, UNIT // BLOCK)),
                dma,
                dma((slots,)),
                dma((slots, 2, ns // 2)),
                dma((slots,)),
                dma((slots,)),
                dma((slots,)),
                dma((slots,)),
                dma((2,)),
                dma((2, 2, parts * (ns - 1) // 2)),
            ],
            compiler_params=pltpu.CompilerParams(collective_id=0, has_side_effects=True, vmem_limit_bytes=67043328),
        )(x, gain, rate[None], wq, wk, wv, wo)

    tokens, rows = P(("dp", "sp"), None), P("sp", None)
    return jax.shard_map(step, mesh=mesh, in_specs=(tokens, P(None), rows, rows, rows, rows), out_specs=tokens, check_vma=False)
```

```python
import functools
import math

import jax
import jax.numpy as jnp
from jax import lax
from jax.experimental import pallas as pl
from jax.experimental.pallas import tpu as pltpu
from jax.sharding import PartitionSpec as P

HEAD = 256
THETA = 10000
NEG = -1e30
HIDDEN = 2 * NEG
LOG2E = 1.4426950408889634
MESH = pl.DeviceIdType.MESH
f32, bf16 = jnp.float32, jnp.bfloat16

UNIT = 512
BLOCK = 128
PART = 512
START = {0: 0, 2: 0, 1: 1, 3: 1, 4: 2}
OUT_HOPS = (2, 6, 9, 11, 13)
KV_WAITS = ((0, 1), (2, 2), (4, 3), (8, 4), (8, 5), (12, 6))
KV_STARTS = ((0, 3), (2, 4), (4, 5), (9, 6))
ALONG_X = (0, 1, 4, 7, 8)


def _dot(a, b, ca=1, cb=0):
    return lax.dot_general(a, b, (((ca,), (cb,)), ((), ())), preferred_element_type=f32)


def _fused(ns, ny, nq, x_hbm, gain_ref, rate_ref, wq_hbm, wk_hbm, wv_hbm, wo_hbm, out_hbm,
           a_s, q_s, k_s, v_s, w_s, mix_s, top_s, cos_s, sin_s, x_sem, load_sem, out_sem, z_send, z_recv, y_send, y_recv, c_send, c_recv,
           kv_send, kv_recv):
    own, width = a_s.shape
    rows = wq_hbm.shape[0]
    parts = own // PART
    nh = q_s.shape[2] // PART
    nu = nq // UNIT
    far, near = ns // 2, ns - 1 - ns // 2
    z, g = lax.axis_index("sp"), lax.axis_index("dp")
    core, yp = lax.rem(g, 2), lax.rem(lax.div(g, 2), 2)
    right, left = {"sp": lax.rem(z + 1, ns)}, {"sp": lax.rem(z + ns - 1, ns)}
    twin = {"dp": g + 1 - 2 * core}
    xp = lax.rem(lax.div(g, 2 * ny), 2)
    pairs = {"y": ({"dp": g + 2 - 4 * yp}, yp), "x": ({"dp": g + (2 - 4 * xp) * ny}, xp)}

    def pair(u):
        return pairs["x" if u in ALONG_X else "y"]

    def at(d):
        return lax.rem(z + d + ns, ns)

    def piece(u, k, s):
        return w_s.at[u, pl.ds(pl.multiple_of(s * rows, rows), rows), pl.ds(pl.multiple_of(k * BLOCK, BLOCK), BLOCK)]

    def send(src, dst, s_sem, r_sem, to):
        return pltpu.make_async_remote_copy(src_ref=src, dst_ref=dst, send_sem=s_sem, recv_sem=r_sem, device_id=to, device_id_type=MESH)

    def slots(u):
        r, l = (far, near) if u % 2 else (near, far)
        return [(u, u, 2 * pair(u)[1] + core, r, l)]

    def hop(slot, u, k, h, way):
        s = at(1 - h) if way == 0 else at(h - 1)
        return send(piece(u, k, s), piece(u, k, s), z_send.at[slot], z_recv.at[slot, way, h - 1], right if way == 0 else left)

    def came(slot, u, k, h, way):
        s = at(-h) if way == 0 else at(h)
        p = piece(u, k, s)
        return send(p, p, z_send.at[slot], z_recv.at[slot, way, h - 1], right), p

    def ring_send(u, h):
        for slot, u, k, r, l in slots(u):
            if h <= r:
                hop(slot, u, k, h, 0).start()
            if h <= l:
                hop(slot, u, k, h, 1).start()

    def hand_on(u, p):
        send(p, p, y_send.at[u], y_recv.at[u], pair(u)[0]).start()
        send(p, p, c_send.at[u], c_recv.at[u], twin).start()

    def ring_step(u, h):
        for slot, u, k, r, l in slots(u):
            for way, n in ((0, r), (1, l)):
                if h <= n:
                    c, p = came(slot, u, k, h, way)
                    c.wait_recv()
                    if h < n:
                        hop(slot, u, k, h + 1, way).start()
                    hand_on(u, p)

    def bulk(u, pieces):
        return w_s.at[u, pl.ds(0, pieces * rows // 2), pl.ds(0, 2 * BLOCK)]

    def from_pair(u):
        send(bulk(u, ns - 1), bulk(u, ns - 1), y_send.at[u], y_recv.at[u], pair(u)[0]).wait_recv()
        k = 2 * (1 - pair(u)[1]) + core
        for d in range(1, ns):
            p = piece(u, k, at(d))
            send(p, p, c_send.at[u], c_recv.at[u], twin).start()

    def whole(u):
        send(bulk(u, 2 * (ns - 1)), bulk(u, 2 * (ns - 1)), c_send.at[u], c_recv.at[u], twin).wait_recv()

    def sent(u):
        for slot, *_ in slots(u):
            send(bulk(u, ns - 1), bulk(u, ns - 1), z_send.at[slot], z_recv.at[slot, 0, 0], right).wait_send()
        send(bulk(u, ns - 1), bulk(u, ns - 1), y_send.at[u], y_recv.at[u], pair(u)[0]).wait_send()
        send(bulk(u, 2 * (ns - 1)), bulk(u, 2 * (ns - 1)), c_send.at[u], c_recv.at[u], twin).wait_send()

    def kv_copies(a, way, s):
        p = lax.rem(a + way, 2)
        to = right if way == 0 else left
        return [send(ref.at[s, p], ref.at[s, p], kv_send.at[i], kv_recv.at[i, way, a], to) for i, ref in enumerate((k_s, v_s))]

    def kv_start(a):
        h = lax.div(a, 2) + 1
        for way, s in ((0, at(1 - h)), (1, at(h - 1))):
            for c in kv_copies(a, way, s):
                c.start()

    def kv_wait(a):
        h = lax.div(a, 2) + 1
        for way, s in ((0, at(-h)), (1, at(h))):
            for c in kv_copies(a, way, s):
                c.wait_recv()

    kv_rounds = parts * (ns - 1) // 2

    def load(u, k):
        if u == 0:
            src, c = (wk_hbm, k) if k < 2 else (wv_hbm, k - 2)
        elif u <= nu:
            src, c = wq_hbm, 4 * (u - 1) + k
        else:
            src, c = wo_hbm, 4 * (u - 1 - nu) + k
        return pltpu.make_async_copy(src.at[:, pl.ds(c * BLOCK, BLOCK)], piece(u, k, z), load_sem.at[u, k])

    units = range(1 + 2 * nu)
    blocks = UNIT // BLOCK
    xt = own // x_sem.shape[0]
    xs = [pltpu.make_async_copy(x_hbm.at[pl.ds(t * xt, xt)], a_s.at[pl.ds(t * xt, xt)], x_sem.at[t]) for t in range(x_sem.shape[0])]
    for k in range(blocks):
        load(0, k).start()
    for c in xs:
        c.start()
    for u in units[1:]:
        for k in range(blocks):
            load(u, k).start()

    barrier = pltpu.get_barrier_semaphore()
    for to in (left, right, twin, pairs["x"][0], pairs["y"][0]):
        pl.semaphore_signal(barrier, inc=1, device_id=to, device_id_type=MESH)
    pl.semaphore_wait(barrier, 5)

    def loaded(u):
        for k in range(blocks):
            load(u, k).wait()

    for u, start in START.items():
        if start == 0:
            loaded(u)
            ring_send(u, 1)

    def norm(t, _):
        r = pl.ds(pl.multiple_of(t * 128, 128), 128)
        wide = a_s[r, :].astype(f32)
        scale = lax.rsqrt(jnp.mean(wide * wide, -1, keepdims=True) + 1e-6)
        a_s[r, :] = (wide * scale * gain_ref[...].astype(f32)[None]).astype(bf16)

    top_s[...] = jnp.full(top_s.shape, NEG, f32)

    def clear(i, _):
        mix_s[lax.div(i, nh), :, pl.ds(pl.multiple_of(lax.rem(i, nh) * PART, PART), PART)] = jnp.zeros((mix_s.shape[1], PART), f32)


    def angles(t, _):
        r = pl.ds(pl.multiple_of(t * 128, 128), 128)
        place = z * own + t * 128 + lax.broadcasted_iota(jnp.int32, (128, HEAD // 2), 0)
        angle = place.astype(f32) * rate_ref[...]
        cos_s[r, :] = jnp.cos(angle)
        sin_s[r, :] = jnp.sin(angle)


    def turned(t, r):
        half = HEAD // 2
        c, s = cos_s[r, :], sin_s[r, :]
        t = t.astype(bf16).astype(f32)
        a, b = t[:, :half], t[:, half:]
        return jnp.concatenate([a * c - b * s, b * c + a * s], axis=1).astype(bf16)

    def keys_values():
        def one(p, _):
            r = pl.ds(pl.multiple_of(p * PART, PART), PART)
            t = _dot(a_s[r, :], w_s[0])
            k_s[z, p] = turned(t[:, :HEAD], r)
            v_s[z, p] = t[:, HEAD:].T.astype(bf16)

        lax.fori_loop(0, parts, one, None)

    def queries(u):
        def one(p, _):
            r = pl.ds(pl.multiple_of(p * PART, PART), PART)
            t = _dot(a_s[r, :], w_s[u])
            for i in range(UNIT // HEAD):
                head = (u - 1) * (UNIT // HEAD) + i
                q_s[p, :, head * PART : (head + 1) * PART] = turned(t[:, i * HEAD : (i + 1) * HEAD], r).astype(f32).T.astype(bf16)

        lax.fori_loop(0, parts, one, None)

    e = HEAD**-0.5 * LOG2E

    cuts = [pl.ds(h * PART, PART) for h in range(nh)]

    def tile(s, n, iq, masked):
        key = k_s[s, 0:n].reshape(n * PART, HEAD)
        value = jnp.concatenate([v_s[s, p] for p in range(n)], axis=1)
        value = jnp.concatenate([value, jnp.ones((8, n * PART), bf16)], axis=0)
        if masked:
            seen = iq * PART + lax.broadcasted_iota(jnp.int32, (n * PART, PART), 1) >= lax.broadcasted_iota(jnp.int32, (n * PART, PART), 0)
        scores, weights = {}, {}
        for i in range(nh + 2):
            if i < nh:
                scores[i] = _dot(key, q_s[iq, :, cuts[i]])
            j = i - 1
            if 0 <= j < nh:
                c, sc = cuts[j], scores.pop(j)
                if masked:
                    sc = jnp.where(seen, sc, HIDDEN)
                old = top_s[iq, :, c]
                top = jnp.maximum(old, sc.max(axis=0, keepdims=True))
                top_s[iq, :, c] = top
                weights[j] = jnp.exp2((sc - top) * e).astype(bf16), jnp.exp2((old - top) * e)
            j = i - 2
            if 0 <= j < nh:
                c, (w, keep) = cuts[j], weights.pop(j)
                mix_s[iq, :, c] = mix_s[iq, :, c] * keep + _dot(value, w)

    rounds = max(START.values()) + far
    for r in range(1, rounds + 1):
        for u, start in START.items():
            if start == r:
                loaded(u)
                ring_send(u, 1)
            elif 1 <= r - start <= far:
                ring_step(u, r - start)
        if r == 1:
            for c in xs:
                c.wait()
            lax.fori_loop(0, own // 128, norm, None)
        if r == 2:
            lax.fori_loop(0, own // 128, angles, None)
        if r == 3:
            lax.fori_loop(0, parts * nh, clear, None)
        if r == far:
            from_pair(0)
        if r == far + 1:
            whole(0)
            keys_values()
            kv_start(0)
            kv_start(1)
    from_pair(2)
    from_pair(1)
    whole(2)
    queries(2)
    from_pair(3)
    whole(1)
    queries(1)
    from_pair(4)
    whole(3)
    queries(3)
    whole(4)
    queries(4)

    for p in range(parts):
        tile(z, p + 1, p, True)

    half = own
    per = w_s.shape[1] // half

    def x_place(c):
        return w_s.at[1 + c // per, pl.ds((c % per) * half, half)]

    again = [pltpu.make_async_copy(x_hbm.at[:, pl.ds(c * UNIT, UNIT)], x_place(c), load_sem.at[1 + c // blocks, c % blocks]) for c in range(width // UNIT)]
    for u in range(1, 1 + len(again) // per):
        sent(u)
    for u in range(1 + nu, 1 + 2 * nu):
        loaded(u)
    for c in again:
        c.start()

    outs = range(1 + nu, 1 + 2 * nu)

    def out_hop(h):
        for u in outs:
            if h:
                ring_step(u, h)
            else:
                ring_send(u, 1)

    def step(t, _):
        a, iq = lax.div(t, parts), lax.rem(t, parts)
        for when, r in KV_WAITS:
            pl.when(t == when)(functools.partial(kv_wait, r))

        for h, when in enumerate(OUT_HOPS):
            pl.when(t == when)(functools.partial(out_hop, h))

        for when, r in KV_STARTS:
            pl.when(t == when)(functools.partial(kv_start, r))

        h = lax.div(a, 2) + 1
        s = jnp.where(lax.rem(a, 2) == 0, at(-h), at(h))

        @pl.when(s < z)
        def _():
            tile(s, parts, iq, False)

    kv_wait(0)
    kv_start(2)
    lax.fori_loop(0, parts * kv_rounds, step, None)

    def finish(p, _):
        r = pl.ds(pl.multiple_of(p * PART, PART), PART)
        for h in range(nh):
            c = pl.ds(h * PART, PART)
            a_s[r, h * HEAD : (h + 1) * HEAD] = (mix_s[p, :HEAD, c] * (1 / mix_s[p, HEAD : HEAD + 1, c])).T.astype(bf16)

    lax.fori_loop(0, parts, finish, None)
    for c in again:
        c.wait()
    for u in outs:
        from_pair(u)
    for u in outs:
        whole(u)

    def result(i, _):
        c, p = lax.div(i, parts), lax.rem(i, parts)
        r = pl.ds(pl.multiple_of(p * PART, PART), PART)
        place = w_s.at[1 + lax.div(c, per), pl.ds(pl.multiple_of(lax.rem(c, per) * half + p * PART, PART), PART)]
        place[...] = (place[...].astype(f32) + _dot(a_s[r, :], w_s[1 + nu + c])).astype(bf16)
        pltpu.make_async_copy(place, out_hbm.at[r, pl.ds(pl.multiple_of(c * UNIT, UNIT), UNIT)], out_sem).start()

    lax.fori_loop(0, parts * (width // UNIT), result, None)

    for u in units:
        if u == 0 or u > len(again) // per:
            sent(u)
    for i, ref in enumerate((k_s, v_s)):
        send(ref.at[pl.ds(0, ns - 1)], ref.at[pl.ds(0, ns - 1)], kv_send.at[i], kv_recv.at[i, 0, 0], right).wait_send()
    pltpu.make_async_copy(a_s, out_hbm, out_sem).wait()


def solution(mesh):
    ns = mesh.shape["sp"]
    ny = math.isqrt(mesh.shape["dp"] // 2)

    def step(x, gain, wq, wk, wv, wo):
        own, width = x.shape
        nq = wq.shape[1]
        nh = nq // HEAD
        nu = nq // UNIT
        parts = own // PART
        half = HEAD // 2
        rate = THETA ** (-jnp.arange(half, dtype=f32) / half)
        anywhere = pl.BlockSpec(memory_space=pl.ANY)
        vmem = pl.BlockSpec(memory_space=pltpu.VMEM)
        dma = pltpu.SemaphoreType.DMA
        slots = 1 + 2 * nu
        return pl.pallas_call(
            functools.partial(_fused, ns, ny, nq),
            out_shape=jax.ShapeDtypeStruct(x.shape, x.dtype),
            in_specs=[anywhere, vmem, vmem] + [anywhere] * 4,
            out_specs=anywhere,
            scratch_shapes=[
                pltpu.VMEM((own, width), bf16),
                pltpu.VMEM((parts, HEAD, nh * PART), bf16),
                pltpu.VMEM((ns, parts, PART, HEAD), bf16),
                pltpu.VMEM((ns, parts, HEAD, PART), bf16),
                pltpu.VMEM((1 + 2 * nu, width, UNIT), bf16),
                pltpu.VMEM((parts, HEAD + 8, nh * PART), f32),
                pltpu.VMEM((parts, 1, nh * PART), f32),
                pltpu.VMEM((own, HEAD // 2), f32),
                pltpu.VMEM((own, HEAD // 2), f32),
                dma((4,)),
                dma((1 + 2 * nu, UNIT // BLOCK)),
                dma,
                dma((slots,)),
                dma((slots, 2, ns // 2)),
                dma((slots,)),
                dma((slots,)),
                dma((slots,)),
                dma((slots,)),
                dma((2,)),
                dma((2, 2, parts * (ns - 1) // 2)),
            ],
            compiler_params=pltpu.CompilerParams(collective_id=0, has_side_effects=True, vmem_limit_bytes=67043328),
        )(x, gain, rate[None], wq, wk, wv, wo)

    tokens, rows = P(("dp", "sp"), None), P("sp", None)
    return jax.shard_map(step, mesh=mesh, in_specs=(tokens, P(None), rows, rows, rows, rows), out_specs=tokens, check_vma=False)
```

```python
import functools
import math

import jax
import jax.numpy as jnp
from jax import lax
from jax.experimental import pallas as pl
from jax.experimental.pallas import tpu as pltpu
from jax.sharding import PartitionSpec as P

HEAD = 256
THETA = 10000
NEG = -1e30
HIDDEN = 2 * NEG
LOG2E = 1.4426950408889634
MESH = pl.DeviceIdType.MESH
f32, bf16 = jnp.float32, jnp.bfloat16

UNIT = 512
BLOCK = 128
PART = 512
START = {0: 0, 2: 0, 1: 0, 3: 1, 4: 1}
OUT_HOPS = (2, 6, 9, 11, 13)
KV_WAITS = ((0, 1), (2, 2), (4, 3), (8, 4), (8, 5), (12, 6))
KV_STARTS = ((0, 3), (2, 4), (4, 5), (9, 6))
ALONG_X = (0, 1, 7, 8)


def _dot(a, b, ca=1, cb=0):
    return lax.dot_general(a, b, (((ca,), (cb,)), ((), ())), preferred_element_type=f32)


def _fused(ns, ny, nq, x_hbm, gain_ref, rate_ref, wq_hbm, wk_hbm, wv_hbm, wo_hbm, out_hbm,
           a_s, q_s, k_s, v_s, w_s, mix_s, top_s, cos_s, sin_s, x_sem, load_sem, out_sem, z_send, z_recv, y_send, y_recv, c_send, c_recv,
           kv_send, kv_recv):
    own, width = a_s.shape
    rows = wq_hbm.shape[0]
    parts = own // PART
    nh = q_s.shape[2] // PART
    nu = nq // UNIT
    far, near = ns // 2, ns - 1 - ns // 2
    z, g = lax.axis_index("sp"), lax.axis_index("dp")
    core, yp = lax.rem(g, 2), lax.rem(lax.div(g, 2), 2)
    right, left = {"sp": lax.rem(z + 1, ns)}, {"sp": lax.rem(z + ns - 1, ns)}
    twin = {"dp": g + 1 - 2 * core}
    xp = lax.rem(lax.div(g, 2 * ny), 2)
    pairs = {"y": ({"dp": g + 2 - 4 * yp}, yp), "x": ({"dp": g + (2 - 4 * xp) * ny}, xp)}

    def pair(u):
        return pairs["x" if u in ALONG_X else "y"]

    def at(d):
        return lax.rem(z + d + ns, ns)

    def piece(u, k, s):
        return w_s.at[u, pl.ds(pl.multiple_of(s * rows, rows), rows), pl.ds(pl.multiple_of(k * BLOCK, BLOCK), BLOCK)]

    def send(src, dst, s_sem, r_sem, to):
        return pltpu.make_async_remote_copy(src_ref=src, dst_ref=dst, send_sem=s_sem, recv_sem=r_sem, device_id=to, device_id_type=MESH)

    def slots(u):
        r, l = (far, near) if u % 2 else (near, far)
        return [(u, u, 2 * pair(u)[1] + core, r, l)]

    def hop(slot, u, k, h, way):
        s = at(1 - h) if way == 0 else at(h - 1)
        return send(piece(u, k, s), piece(u, k, s), z_send.at[slot], z_recv.at[slot, way, h - 1], right if way == 0 else left)

    def came(slot, u, k, h, way):
        s = at(-h) if way == 0 else at(h)
        p = piece(u, k, s)
        return send(p, p, z_send.at[slot], z_recv.at[slot, way, h - 1], right), p

    def ring_send(u, h):
        for slot, u, k, r, l in slots(u):
            if h <= r:
                hop(slot, u, k, h, 0).start()
            if h <= l:
                hop(slot, u, k, h, 1).start()

    def hand_on(u, p):
        send(p, p, y_send.at[u], y_recv.at[u], pair(u)[0]).start()
        send(p, p, c_send.at[u], c_recv.at[u], twin).start()

    def ring_step(u, h):
        for slot, u, k, r, l in slots(u):
            for way, n in ((0, r), (1, l)):
                if h <= n:
                    c, p = came(slot, u, k, h, way)
                    c.wait_recv()
                    if h < n:
                        hop(slot, u, k, h + 1, way).start()
                    hand_on(u, p)

    def bulk(u, pieces):
        return w_s.at[u, pl.ds(0, pieces * rows // 2), pl.ds(0, 2 * BLOCK)]

    def from_pair(u):
        send(bulk(u, ns - 1), bulk(u, ns - 1), y_send.at[u], y_recv.at[u], pair(u)[0]).wait_recv()
        k = 2 * (1 - pair(u)[1]) + core
        for d in range(1, ns):
            p = piece(u, k, at(d))
            send(p, p, c_send.at[u], c_recv.at[u], twin).start()

    def whole(u):
        send(bulk(u, 2 * (ns - 1)), bulk(u, 2 * (ns - 1)), c_send.at[u], c_recv.at[u], twin).wait_recv()

    def sent(u):
        for slot, *_ in slots(u):
            send(bulk(u, ns - 1), bulk(u, ns - 1), z_send.at[slot], z_recv.at[slot, 0, 0], right).wait_send()
        send(bulk(u, ns - 1), bulk(u, ns - 1), y_send.at[u], y_recv.at[u], pair(u)[0]).wait_send()
        send(bulk(u, 2 * (ns - 1)), bulk(u, 2 * (ns - 1)), c_send.at[u], c_recv.at[u], twin).wait_send()

    def kv_copies(a, way, s):
        p = lax.rem(a + way, 2)
        to = right if way == 0 else left
        return [send(ref.at[s, p], ref.at[s, p], kv_send.at[i], kv_recv.at[i, way, a], to) for i, ref in enumerate((k_s, v_s))]

    def kv_start(a):
        h = lax.div(a, 2) + 1
        for way, s in ((0, at(1 - h)), (1, at(h - 1))):
            for c in kv_copies(a, way, s):
                c.start()

    def kv_wait(a):
        h = lax.div(a, 2) + 1
        for way, s in ((0, at(-h)), (1, at(h))):
            for c in kv_copies(a, way, s):
                c.wait_recv()

    kv_rounds = parts * (ns - 1) // 2

    def load(u, k):
        if u == 0:
            src, c = (wk_hbm, k) if k < 2 else (wv_hbm, k - 2)
        elif u <= nu:
            src, c = wq_hbm, 4 * (u - 1) + k
        else:
            src, c = wo_hbm, 4 * (u - 1 - nu) + k
        return pltpu.make_async_copy(src.at[:, pl.ds(c * BLOCK, BLOCK)], piece(u, k, z), load_sem.at[u, k])

    units = range(1 + 2 * nu)
    blocks = UNIT // BLOCK
    xt = own // x_sem.shape[0]
    xs = [pltpu.make_async_copy(x_hbm.at[pl.ds(t * xt, xt)], a_s.at[pl.ds(t * xt, xt)], x_sem.at[t]) for t in range(x_sem.shape[0])]
    for k in range(blocks):
        load(0, k).start()
    for c in xs:
        c.start()
    for u in units[1:]:
        for k in range(blocks):
            load(u, k).start()

    barrier = pltpu.get_barrier_semaphore()
    for to in (left, right, twin, pairs["x"][0], pairs["y"][0]):
        pl.semaphore_signal(barrier, inc=1, device_id=to, device_id_type=MESH)
    pl.semaphore_wait(barrier, 5)

    def loaded(u):
        for k in range(blocks):
            load(u, k).wait()

    for u, start in START.items():
        if start == 0:
            loaded(u)
            ring_send(u, 1)

    def norm(t, _):
        r = pl.ds(pl.multiple_of(t * 128, 128), 128)
        wide = a_s[r, :].astype(f32)
        scale = lax.rsqrt(jnp.mean(wide * wide, -1, keepdims=True) + 1e-6)
        a_s[r, :] = (wide * scale * gain_ref[...].astype(f32)[None]).astype(bf16)

    top_s[...] = jnp.full(top_s.shape, NEG, f32)

    def clear(i, _):
        mix_s[lax.div(i, nh), :, pl.ds(pl.multiple_of(lax.rem(i, nh) * PART, PART), PART)] = jnp.zeros((mix_s.shape[1], PART), f32)


    def angles(t, _):
        r = pl.ds(pl.multiple_of(t * 128, 128), 128)
        place = z * own + t * 128 + lax.broadcasted_iota(jnp.int32, (128, HEAD // 2), 0)
        angle = place.astype(f32) * rate_ref[...]
        cos_s[r, :] = jnp.cos(angle)
        sin_s[r, :] = jnp.sin(angle)


    def turned(t, r):
        half = HEAD // 2
        c, s = cos_s[r, :], sin_s[r, :]
        t = t.astype(bf16).astype(f32)
        a, b = t[:, :half], t[:, half:]
        return jnp.concatenate([a * c - b * s, b * c + a * s], axis=1).astype(bf16)

    def keys_values(p):
        r = pl.ds(p * PART, PART)
        t = _dot(a_s[r, :], w_s[0])
        k_s[z, p] = turned(t[:, :HEAD], r)
        v_s[z, p] = t[:, HEAD:].T.astype(bf16)

    def queries(u):
        def one(p, _):
            r = pl.ds(pl.multiple_of(p * PART, PART), PART)
            t = _dot(a_s[r, :], w_s[u])
            for i in range(UNIT // HEAD):
                head = (u - 1) * (UNIT // HEAD) + i
                q_s[p, :, head * PART : (head + 1) * PART] = turned(t[:, i * HEAD : (i + 1) * HEAD], r).astype(f32).T.astype(bf16)

        lax.fori_loop(0, parts, one, None)

    e = HEAD**-0.5 * LOG2E

    cuts = [pl.ds(h * PART, PART) for h in range(nh)]

    def tile(s, n, iq, masked):
        key = k_s[s, 0:n].reshape(n * PART, HEAD)
        value = jnp.concatenate([v_s[s, p] for p in range(n)], axis=1)
        value = jnp.concatenate([value, jnp.ones((8, n * PART), bf16)], axis=0)
        if masked:
            seen = iq * PART + lax.broadcasted_iota(jnp.int32, (n * PART, PART), 1) >= lax.broadcasted_iota(jnp.int32, (n * PART, PART), 0)
        scores, weights = {}, {}
        for i in range(nh + 2):
            if i < nh:
                scores[i] = _dot(key, q_s[iq, :, cuts[i]])
            j = i - 1
            if 0 <= j < nh:
                c, sc = cuts[j], scores.pop(j)
                if masked:
                    sc = jnp.where(seen, sc, HIDDEN)
                old = top_s[iq, :, c]
                top = jnp.maximum(old, sc.max(axis=0, keepdims=True))
                top_s[iq, :, c] = top
                weights[j] = jnp.exp2((sc - top) * e).astype(bf16), jnp.exp2((old - top) * e)
            j = i - 2
            if 0 <= j < nh:
                c, (w, keep) = cuts[j], weights.pop(j)
                mix_s[iq, :, c] = mix_s[iq, :, c] * keep + _dot(value, w)

    rounds = max(START.values()) + far
    for r in range(1, rounds + 1):
        for u, start in START.items():
            if start == r:
                loaded(u)
                ring_send(u, 1)
            elif 1 <= r - start <= far:
                ring_step(u, r - start)
        if r == 1:
            for c in xs:
                c.wait()
            lax.fori_loop(0, own // 128, norm, None)
        if r == 2:
            lax.fori_loop(0, own // 128, angles, None)
        if r == 3:
            lax.fori_loop(0, parts * nh, clear, None)
        if r == far:
            from_pair(0)
            whole(0)
            for p in range(parts):
                keys_values(p)
                if p == 0:
                    from_pair(1)
            kv_start(0)
            kv_start(1)
    from_pair(2)
    whole(1)
    queries(1)
    whole(2)
    queries(2)
    from_pair(3)
    from_pair(4)
    whole(3)
    queries(3)
    whole(4)
    queries(4)
    kv_wait(0)
    kv_start(2)

    for p in range(parts):
        tile(z, p + 1, p, True)

    half = own
    per = w_s.shape[1] // half

    def x_place(c):
        return w_s.at[1 + c // per, pl.ds((c % per) * half, half)]

    again = [pltpu.make_async_copy(x_hbm.at[:, pl.ds(c * UNIT, UNIT)], x_place(c), load_sem.at[1 + c // blocks, c % blocks]) for c in range(width // UNIT)]
    for u in range(1, 1 + len(again) // per):
        sent(u)
    for u in range(1 + nu, 1 + 2 * nu):
        loaded(u)
    for c in again:
        c.start()

    outs = range(1 + nu, 1 + 2 * nu)

    def out_hop(h):
        for u in outs:
            if h:
                ring_step(u, h)
            else:
                ring_send(u, 1)

    def step(t, _):
        a, iq = lax.div(t, parts), lax.rem(t, parts)
        for when, r in KV_WAITS:
            pl.when(t == when)(functools.partial(kv_wait, r))

        for h, when in enumerate(OUT_HOPS):
            pl.when(t == when)(functools.partial(out_hop, h))

        for when, r in KV_STARTS:
            pl.when(t == when)(functools.partial(kv_start, r))

        h = lax.div(a, 2) + 1
        s = jnp.where(lax.rem(a, 2) == 0, at(-h), at(h))

        @pl.when(s < z)
        def _():
            tile(s, parts, iq, False)

    lax.fori_loop(0, parts * kv_rounds, step, None)

    def finish(p, _):
        r = pl.ds(pl.multiple_of(p * PART, PART), PART)
        for h in range(nh):
            c = pl.ds(h * PART, PART)
            a_s[r, h * HEAD : (h + 1) * HEAD] = (mix_s[p, :HEAD, c] * (1 / mix_s[p, HEAD : HEAD + 1, c])).T.astype(bf16)

    for u in outs:
        from_pair(u)
    lax.fori_loop(0, parts, finish, None)
    for c in again:
        c.wait()

    def result(i, _):
        c, p = lax.div(i, parts), lax.rem(i, parts)

        @pl.when(p == 0)
        def _():
            whole(1 + nu + c)

        r = pl.ds(pl.multiple_of(p * PART, PART), PART)
        place = w_s.at[1 + lax.div(c, per), pl.ds(pl.multiple_of(lax.rem(c, per) * half + p * PART, PART), PART)]
        place[...] = (place[...].astype(f32) + _dot(a_s[r, :], w_s[1 + nu + c])).astype(bf16)
        pltpu.make_async_copy(place, out_hbm.at[r, pl.ds(pl.multiple_of(c * UNIT, UNIT), UNIT)], out_sem).start()

    lax.fori_loop(0, parts * (width // UNIT), result, None)

    for u in units:
        if u == 0 or u > len(again) // per:
            sent(u)
    for i, ref in enumerate((k_s, v_s)):
        send(ref.at[pl.ds(0, ns - 1)], ref.at[pl.ds(0, ns - 1)], kv_send.at[i], kv_recv.at[i, 0, 0], right).wait_send()
    pltpu.make_async_copy(a_s, out_hbm, out_sem).wait()


def solution(mesh):
    ns = mesh.shape["sp"]
    ny = math.isqrt(mesh.shape["dp"] // 2)

    def step(x, gain, wq, wk, wv, wo):
        own, width = x.shape
        nq = wq.shape[1]
        nh = nq // HEAD
        nu = nq // UNIT
        parts = own // PART
        half = HEAD // 2
        rate = THETA ** (-jnp.arange(half, dtype=f32) / half)
        anywhere = pl.BlockSpec(memory_space=pl.ANY)
        vmem = pl.BlockSpec(memory_space=pltpu.VMEM)
        dma = pltpu.SemaphoreType.DMA
        slots = 1 + 2 * nu
        return pl.pallas_call(
            functools.partial(_fused, ns, ny, nq),
            out_shape=jax.ShapeDtypeStruct(x.shape, x.dtype),
            in_specs=[anywhere, vmem, vmem] + [anywhere] * 4,
            out_specs=anywhere,
            scratch_shapes=[
                pltpu.VMEM((own, width), bf16),
                pltpu.VMEM((parts, HEAD, nh * PART), bf16),
                pltpu.VMEM((ns, parts, PART, HEAD), bf16),
                pltpu.VMEM((ns, parts, HEAD, PART), bf16),
                pltpu.VMEM((1 + 2 * nu, width, UNIT), bf16),
                pltpu.VMEM((parts, HEAD + 8, nh * PART), f32),
                pltpu.VMEM((parts, 1, nh * PART), f32),
                pltpu.VMEM((own, HEAD // 2), f32),
                pltpu.VMEM((own, HEAD // 2), f32),
                dma((4,)),
                dma((1 + 2 * nu, UNIT // BLOCK)),
                dma,
                dma((slots,)),
                dma((slots, 2, ns // 2)),
                dma((slots,)),
                dma((slots,)),
                dma((slots,)),
                dma((slots,)),
                dma((2,)),
                dma((2, 2, parts * (ns - 1) // 2)),
            ],
            compiler_params=pltpu.CompilerParams(collective_id=0, has_side_effects=True, vmem_limit_bytes=67043328),
        )(x, gain, rate[None], wq, wk, wv, wo)

    tokens, rows = P(("dp", "sp"), None), P("sp", None)
    return jax.shard_map(step, mesh=mesh, in_specs=(tokens, P(None), rows, rows, rows, rows), out_specs=tokens, check_vma=False)
```

```python
import functools
import math

import jax
import jax.numpy as jnp
from jax import lax
from jax.experimental import pallas as pl
from jax.experimental.pallas import tpu as pltpu
from jax.sharding import PartitionSpec as P

HEAD = 256
THETA = 10000
NEG = -3e38
HIDDEN = -jnp.inf
LOG2E = 1.4426950408889634
MESH = pl.DeviceIdType.MESH
f32, bf16 = jnp.float32, jnp.bfloat16

UNIT = 512
BLOCK = 128
PART = 512
START = {0: 0, 2: 0, 1: 0, 3: 1, 4: 1}
OUT_HOPS = (2, 6, 9, 11, 13)
KV_WAITS = ((0, 1), (2, 2), (4, 3), (8, 4), (8, 5), (12, 6))
KV_STARTS = ((0, 3), (2, 4), (4, 5), (9, 6))
ALONG_X = (0, 1, 7, 8)


def _dot(a, b, ca=1, cb=0):
    return lax.dot_general(a, b, (((ca,), (cb,)), ((), ())), preferred_element_type=f32)


def _fused(ns, ny, nq, x_hbm, gain_ref, rate_ref, wq_hbm, wk_hbm, wv_hbm, wo_hbm, out_hbm,
           a_s, q_s, k_s, v_s, w_s, mix_s, top_s, cos_s, sin_s, x_sem, load_sem, out_sem, z_send, z_recv, y_send, y_recv, c_send, c_recv,
           kv_send, kv_recv):
    own, width = a_s.shape
    rows = wq_hbm.shape[0]
    parts = own // PART
    nh = q_s.shape[2] // PART
    nu = nq // UNIT
    far, near = ns // 2, ns - 1 - ns // 2
    z, g = lax.axis_index("sp"), lax.axis_index("dp")
    core, yp = lax.rem(g, 2), lax.rem(lax.div(g, 2), 2)
    right, left = {"sp": lax.rem(z + 1, ns)}, {"sp": lax.rem(z + ns - 1, ns)}
    twin = {"dp": g + 1 - 2 * core}
    xp = lax.rem(lax.div(g, 2 * ny), 2)
    pairs = {"y": ({"dp": g + 2 - 4 * yp}, yp), "x": ({"dp": g + (2 - 4 * xp) * ny}, xp)}

    def pair(u):
        return pairs["x" if u in ALONG_X else "y"]

    def at(d):
        return lax.rem(z + d + ns, ns)

    def piece(u, k, s):
        return w_s.at[u, pl.ds(pl.multiple_of(s * rows, rows), rows), pl.ds(pl.multiple_of(k * BLOCK, BLOCK), BLOCK)]

    def send(src, dst, s_sem, r_sem, to):
        return pltpu.make_async_remote_copy(src_ref=src, dst_ref=dst, send_sem=s_sem, recv_sem=r_sem, device_id=to, device_id_type=MESH)

    def slots(u):
        r, l = (far, near) if u % 2 else (near, far)
        return [(u, u, 2 * pair(u)[1] + core, r, l)]

    def hop(slot, u, k, h, way):
        s = at(1 - h) if way == 0 else at(h - 1)
        return send(piece(u, k, s), piece(u, k, s), z_send.at[slot], z_recv.at[slot, way, h - 1], right if way == 0 else left)

    def came(slot, u, k, h, way):
        s = at(-h) if way == 0 else at(h)
        p = piece(u, k, s)
        return send(p, p, z_send.at[slot], z_recv.at[slot, way, h - 1], right), p

    def ring_send(u, h):
        for slot, u, k, r, l in slots(u):
            if h <= r:
                hop(slot, u, k, h, 0).start()
            if h <= l:
                hop(slot, u, k, h, 1).start()

    def hand_on(u, p):
        send(p, p, y_send.at[u], y_recv.at[u], pair(u)[0]).start()
        send(p, p, c_send.at[u], c_recv.at[u], twin).start()

    def ring_step(u, h):
        for slot, u, k, r, l in slots(u):
            for way, n in ((0, r), (1, l)):
                if h <= n:
                    c, p = came(slot, u, k, h, way)
                    c.wait_recv()
                    if h < n:
                        hop(slot, u, k, h + 1, way).start()
                    hand_on(u, p)

    def bulk(u, pieces):
        return w_s.at[u, pl.ds(0, pieces * rows // 2), pl.ds(0, 2 * BLOCK)]

    def from_pair(u):
        send(bulk(u, ns - 1), bulk(u, ns - 1), y_send.at[u], y_recv.at[u], pair(u)[0]).wait_recv()
        k = 2 * (1 - pair(u)[1]) + core
        for d in range(1, ns):
            p = piece(u, k, at(d))
            send(p, p, c_send.at[u], c_recv.at[u], twin).start()

    def whole(u):
        send(bulk(u, 2 * (ns - 1)), bulk(u, 2 * (ns - 1)), c_send.at[u], c_recv.at[u], twin).wait_recv()

    def sent(u):
        for slot, *_ in slots(u):
            send(bulk(u, ns - 1), bulk(u, ns - 1), z_send.at[slot], z_recv.at[slot, 0, 0], right).wait_send()
        send(bulk(u, ns - 1), bulk(u, ns - 1), y_send.at[u], y_recv.at[u], pair(u)[0]).wait_send()
        send(bulk(u, 2 * (ns - 1)), bulk(u, 2 * (ns - 1)), c_send.at[u], c_recv.at[u], twin).wait_send()

    def kv_copies(a, way, s):
        p = lax.rem(a + way, 2)
        to = right if way == 0 else left
        return [send(ref.at[s, p], ref.at[s, p], kv_send.at[i], kv_recv.at[i, way, a], to) for i, ref in enumerate((k_s, v_s))]

    def kv_start(a):
        h = lax.div(a, 2) + 1
        for way, s in ((0, at(1 - h)), (1, at(h - 1))):
            for c in kv_copies(a, way, s):
                c.start()

    def kv_wait(a):
        h = lax.div(a, 2) + 1
        for way, s in ((0, at(-h)), (1, at(h))):
            for c in kv_copies(a, way, s):
                c.wait_recv()

    kv_rounds = parts * (ns - 1) // 2

    def load(u, k):
        if u == 0:
            src, c = (wk_hbm, k) if k < 2 else (wv_hbm, k - 2)
        elif u <= nu:
            src, c = wq_hbm, 4 * (u - 1) + k
        else:
            src, c = wo_hbm, 4 * (u - 1 - nu) + k
        return pltpu.make_async_copy(src.at[:, pl.ds(c * BLOCK, BLOCK)], piece(u, k, z), load_sem.at[u, k])

    units = range(1 + 2 * nu)
    blocks = UNIT // BLOCK
    xt = own // x_sem.shape[0]
    xs = [pltpu.make_async_copy(x_hbm.at[pl.ds(t * xt, xt)], a_s.at[pl.ds(t * xt, xt)], x_sem.at[t]) for t in range(x_sem.shape[0])]
    for k in range(blocks):
        load(0, k).start()
    for c in xs:
        c.start()
    for u in units[1:]:
        for k in range(blocks):
            load(u, k).start()

    barrier = pltpu.get_barrier_semaphore()
    for to in (left, right, twin, pairs["x"][0], pairs["y"][0]):
        pl.semaphore_signal(barrier, inc=1, device_id=to, device_id_type=MESH)
    pl.semaphore_wait(barrier, 5)

    def loaded(u):
        for k in range(blocks):
            load(u, k).wait()

    for u, start in START.items():
        if start == 0:
            loaded(u)
            ring_send(u, 1)

    def norm(t, _):
        r = pl.ds(pl.multiple_of(t * 128, 128), 128)
        wide = a_s[r, :].astype(f32)
        scale = lax.rsqrt(jnp.mean(wide * wide, -1, keepdims=True) + 1e-6)
        a_s[r, :] = (wide * scale * gain_ref[...].astype(f32)[None]).astype(bf16)

    top_s[...] = jnp.full(top_s.shape, NEG, f32)

    def clear(i, _):
        mix_s[lax.div(i, nh), :, pl.ds(pl.multiple_of(lax.rem(i, nh) * PART, PART), PART)] = jnp.zeros((mix_s.shape[1], PART), f32)


    def angles(t, _):
        r = pl.ds(pl.multiple_of(t * 128, 128), 128)
        place = z * own + t * 128 + lax.broadcasted_iota(jnp.int32, (128, HEAD // 2), 0)
        angle = place.astype(f32) * rate_ref[...]
        cos_s[r, :] = jnp.cos(angle)
        sin_s[r, :] = jnp.sin(angle)


    def turned(t, r):
        half = HEAD // 2
        c, s = cos_s[r, :], sin_s[r, :]
        t = t.astype(bf16).astype(f32)
        a, b = t[:, :half], t[:, half:]
        return jnp.concatenate([a * c - b * s, b * c + a * s], axis=1).astype(bf16)

    def keys_values(p):
        r = pl.ds(p * PART, PART)
        t = _dot(a_s[r, :], w_s[0])
        k_s[z, p] = turned(t[:, :HEAD], r)
        v_s[z, p] = t[:, HEAD:].T.astype(bf16)

    def queries(u):
        def one(p, _):
            r = pl.ds(pl.multiple_of(p * PART, PART), PART)
            t = _dot(a_s[r, :], w_s[u])
            for i in range(UNIT // HEAD):
                head = (u - 1) * (UNIT // HEAD) + i
                q_s[p, :, head * PART : (head + 1) * PART] = turned(t[:, i * HEAD : (i + 1) * HEAD], r).astype(f32).T.astype(bf16)

        lax.fori_loop(0, parts, one, None)

    e = HEAD**-0.5 * LOG2E

    cuts = [pl.ds(h * PART, PART) for h in range(nh)]

    def tile(s, n, iq, masked):
        key = k_s[s, 0:n].reshape(n * PART, HEAD)
        value = jnp.concatenate([v_s[s, p] for p in range(n)], axis=1)
        value = jnp.concatenate([value, jnp.ones((8, n * PART), bf16)], axis=0)
        if masked:
            seen = iq * PART + lax.broadcasted_iota(jnp.int32, (n * PART, PART), 1) >= lax.broadcasted_iota(jnp.int32, (n * PART, PART), 0)
        scores, weights = {}, {}
        for i in range(nh + 2):
            if i < nh:
                scores[i] = _dot(key, q_s[iq, :, cuts[i]])
            j = i - 1
            if 0 <= j < nh:
                c, sc = cuts[j], scores.pop(j)
                if masked:
                    sc = jnp.where(seen, sc, HIDDEN)
                old = top_s[iq, :, c]
                top = jnp.maximum(old, sc.max(axis=0, keepdims=True))
                top_s[iq, :, c] = top
                weights[j] = jnp.exp2((sc - top) * e).astype(bf16), jnp.exp2((old - top) * e)
            j = i - 2
            if 0 <= j < nh:
                c, (w, keep) = cuts[j], weights.pop(j)
                mix_s[iq, :, c] = mix_s[iq, :, c] * keep + _dot(value, w)

    rounds = max(START.values()) + far
    for r in range(1, rounds + 1):
        for u, start in START.items():
            if start == r:
                loaded(u)
                ring_send(u, 1)
            elif 1 <= r - start <= far:
                ring_step(u, r - start)
        if r == 1:
            for c in xs:
                c.wait()
            lax.fori_loop(0, own // 128, norm, None)
        if r == 2:
            lax.fori_loop(0, own // 128, angles, None)
        if r == 3:
            lax.fori_loop(0, parts * nh, clear, None)
        if r == far:
            from_pair(0)
            whole(0)
            for p in range(parts):
                keys_values(p)
                if p == 0:
                    from_pair(1)
            kv_start(0)
            kv_start(1)
    from_pair(2)
    whole(1)
    queries(1)
    whole(2)
    queries(2)
    from_pair(3)
    from_pair(4)
    whole(3)
    queries(3)
    whole(4)
    queries(4)
    kv_wait(0)
    kv_start(2)

    for p in range(parts):
        tile(z, p + 1, p, True)

    half = own
    per = w_s.shape[1] // half

    def x_place(c):
        return w_s.at[1 + c // per, pl.ds((c % per) * half, half)]

    again = [pltpu.make_async_copy(x_hbm.at[:, pl.ds(c * UNIT, UNIT)], x_place(c), load_sem.at[1 + c // blocks, c % blocks]) for c in range(width // UNIT)]
    for u in range(1, 1 + len(again) // per):
        sent(u)
    for u in range(1 + nu, 1 + 2 * nu):
        loaded(u)
    for c in again:
        c.start()

    outs = range(1 + nu, 1 + 2 * nu)

    def out_hop(h):
        for u in outs:
            if h:
                ring_step(u, h)
            else:
                ring_send(u, 1)

    def step(t, _):
        a, iq = lax.div(t, parts), lax.rem(t, parts)
        for when, r in KV_WAITS:
            pl.when(t == when)(functools.partial(kv_wait, r))

        for h, when in enumerate(OUT_HOPS):
            pl.when(t == when)(functools.partial(out_hop, h))

        for when, r in KV_STARTS:
            pl.when(t == when)(functools.partial(kv_start, r))

        h = lax.div(a, 2) + 1
        s = jnp.where(lax.rem(a, 2) == 0, at(-h), at(h))

        @pl.when(s < z)
        def _():
            tile(s, parts, iq, False)

    lax.fori_loop(0, parts * kv_rounds, step, None)

    def finish(p, _):
        r = pl.ds(pl.multiple_of(p * PART, PART), PART)
        for h in range(nh):
            c = pl.ds(h * PART, PART)
            a_s[r, h * HEAD : (h + 1) * HEAD] = (mix_s[p, :HEAD, c] * (1 / mix_s[p, HEAD : HEAD + 1, c])).T.astype(bf16)

    for u in outs:
        from_pair(u)
    lax.fori_loop(0, parts, finish, None)
    for c in again:
        c.wait()

    def result(i, _):
        c, p = lax.div(i, parts), lax.rem(i, parts)

        @pl.when(p == 0)
        def _():
            whole(1 + nu + c)

        r = pl.ds(pl.multiple_of(p * PART, PART), PART)
        place = w_s.at[1 + lax.div(c, per), pl.ds(pl.multiple_of(lax.rem(c, per) * half + p * PART, PART), PART)]
        place[...] = (place[...].astype(f32) + _dot(a_s[r, :], w_s[1 + nu + c])).astype(bf16)
        pltpu.make_async_copy(place, out_hbm.at[r, pl.ds(pl.multiple_of(c * UNIT, UNIT), UNIT)], out_sem).start()

    lax.fori_loop(0, parts * (width // UNIT), result, None)

    for u in units:
        if u == 0 or u > len(again) // per:
            sent(u)
    for i, ref in enumerate((k_s, v_s)):
        send(ref.at[pl.ds(0, ns - 1)], ref.at[pl.ds(0, ns - 1)], kv_send.at[i], kv_recv.at[i, 0, 0], right).wait_send()
    pltpu.make_async_copy(a_s, out_hbm, out_sem).wait()


def solution(mesh):
    ns = mesh.shape["sp"]
    ny = math.isqrt(mesh.shape["dp"] // 2)

    def step(x, gain, wq, wk, wv, wo):
        own, width = x.shape
        nq = wq.shape[1]
        nh = nq // HEAD
        nu = nq // UNIT
        parts = own // PART
        half = HEAD // 2
        rate = THETA ** (-jnp.arange(half, dtype=f32) / half)
        anywhere = pl.BlockSpec(memory_space=pl.ANY)
        vmem = pl.BlockSpec(memory_space=pltpu.VMEM)
        dma = pltpu.SemaphoreType.DMA
        slots = 1 + 2 * nu
        return pl.pallas_call(
            functools.partial(_fused, ns, ny, nq),
            out_shape=jax.ShapeDtypeStruct(x.shape, x.dtype),
            in_specs=[anywhere, vmem, vmem] + [anywhere] * 4,
            out_specs=anywhere,
            scratch_shapes=[
                pltpu.VMEM((own, width), bf16),
                pltpu.VMEM((parts, HEAD, nh * PART), bf16),
                pltpu.VMEM((ns, parts, PART, HEAD), bf16),
                pltpu.VMEM((ns, parts, HEAD, PART), bf16),
                pltpu.VMEM((1 + 2 * nu, width, UNIT), bf16),
                pltpu.VMEM((parts, HEAD + 8, nh * PART), f32),
                pltpu.VMEM((parts, 1, nh * PART), f32),
                pltpu.VMEM((own, HEAD // 2), f32),
                pltpu.VMEM((own, HEAD // 2), f32),
                dma((4,)),
                dma((1 + 2 * nu, UNIT // BLOCK)),
                dma,
                dma((slots,)),
                dma((slots, 2, ns // 2)),
                dma((slots,)),
                dma((slots,)),
                dma((slots,)),
                dma((slots,)),
                dma((2,)),
                dma((2, 2, parts * (ns - 1) // 2)),
            ],
            compiler_params=pltpu.CompilerParams(collective_id=0, has_side_effects=True, vmem_limit_bytes=67043328),
        )(x, gain, rate[None], wq, wk, wv, wo)

    tokens, rows = P(("dp", "sp"), None), P("sp", None)
    return jax.shard_map(step, mesh=mesh, in_specs=(tokens, P(None), rows, rows, rows, rows), out_specs=tokens, check_vma=False)
```
